32 devices in a mesh: lat: 8 (over z, y), lon: 4 (over x, core).
Axes of the slice: x: 2, y: 2, z: 4, core: 2. Of those that a mesh axis runs over, the one named last changes fastest.
Arguments:
- field: bfloat16 [150, 128, 1024], P(None, 'lat', 'lon'), may hold values from -6 to 6
- land_mask: int32 [128, 1024], P('lat', 'lon'), may hold values 0 or 1
- fold_partner: int32 [1024], replicated, may hold values from 0 to 1023, as said below
- dw_kernel: float32 [150, 7, 7], replicated, may hold values from -0.875 to 0.875
- norm_gain: float32 [150], replicated, may hold values from 0.1 to 1.9
- w_in: bfloat16 [150, 600], replicated, may hold values from -0.5 to 0.5
- w_out: bfloat16 [600, 150], replicated, may hold values from -0.25 to 0.25
- spec_gain: float32 [2, 150, 512], replicated, may hold values from -12 to 12
- mix_weight: bfloat16 [150, 150], replicated, may hold values from -0.5 to 0.5
Outputs:
- block_out: bfloat16 [150, 128, 1024], P(None, 'lat', 'lon')
The draws below stay inside these ranges and needn't reach their ends.
Inputs may be any that keep to these rules, and one draw needn't show every extreme that they name: There is one s such that fold_partner[j] = (s - j) mod 1024 for every j.
All inputs are finite; a program needn't handle non-finite values. No bound on the sum of `land_mask` on one device may be relied on, other than what follows from the above.
Results may differ from the reference program's by a relative error of at most 0.0065.
Values may be sent and summed in bfloat16 or wider, within the bound.
A program may use at most 128 MiB of HBM per device.

```python
import math
import jax
import jax.numpy as jnp
from jax import lax

C = 150
HID = 600
M = 512
RL = 16
NLAT = 128
LON = 1024


def draw_fold_partner(key, part):
    pivot_at = jax.random.randint(jax.random.fold_in(key, 11), (), 0, LON, dtype=jnp.int32)
    return ((pivot_at - jnp.arange(LON, dtype=jnp.int32)) % LON).astype(jnp.int32)


def plant(drawn, stream_key, low, largest):
    spot = [jax.random.randint(jax.random.fold_in(stream_key, axis), (), 0, length) for axis, length in enumerate(drawn.shape)]
    widest = drawn.shape.index(max(drawn.shape))
    neighbour = spot[:widest] + [(spot[widest] + 1) % drawn.shape[widest]] + spot[widest + 1:]
    return drawn.at[tuple(spot)].set(low).at[tuple(neighbour)].set(largest)


def levels(own_key, dims, split, low, top_value):
    gain = 1.0
    for axis_at, blocks in split:
        draws = jax.random.uniform(jax.random.fold_in(jax.random.fold_in(own_key, 6), axis_at), (blocks,), jnp.float32, low / len(split), top_value / len(split))
        gain = gain * jnp.repeat(jnp.exp(draws), dims[axis_at] // blocks).reshape((-1,) + (1,) * (len(dims) - 1 - axis_at))
    return gain


def bell_draw(key, dims, width, bound, shards=(), kind=jnp.bfloat16):
    drawn = width * jax.random.normal(key, dims, jnp.float32)
    if shards:
        drawn = drawn * levels(key, dims, shards, -0.22, 0.18)
    return jnp.clip(drawn, -bound, bound).astype(kind)


def setup_inputs(seed: int = 0) -> dict:
    keys = jax.random.split(jax.random.key(seed), 10)
    field = bell_draw(keys[0], (C, NLAT, LON), 1.0, 6.0, ((1, 8), (2, 4)))
    land_mask = plant((jax.random.randint(keys[1], (NLAT, LON), 0, 4) < 3).astype(jnp.int32), jax.random.fold_in(keys[1], 1), 0, 1)
    fold_partner = draw_fold_partner(jax.random.fold_in(keys[9], 71), 0)
    dw_kernel = bell_draw(keys[3], (C, 7, 7), 49 ** -0.5, 0.875, (), jnp.float32)
    norm_gain = jnp.clip(1.0 + 0.18 * jax.random.normal(keys[4], (C,), jnp.float32), 0.1, 1.9)
    w_in = bell_draw(keys[5], (C, HID), C ** -0.5, 0.5)
    w_out = bell_draw(keys[6], (HID, C), HID ** -0.5, 0.25)
    spec_gain = bell_draw(keys[7], (2, C, M), 2.0, 12.0, (), jnp.float32)
    mix_weight = bell_draw(keys[8], (C, C), C ** -0.5, 0.5)
    return {"field": field, "land_mask": land_mask, "fold_partner": fold_partner, "dw_kernel": dw_kernel, "norm_gain": norm_gain, "w_in": w_in, "w_out": w_out, "spec_gain": spec_gain, "mix_weight": mix_weight}


def dft_table(lon_points, mode_count, first_col, col_count):
    points = first_col + jnp.arange(col_count, dtype=jnp.int32)
    freqs = jnp.arange(mode_count, dtype=jnp.int32)
    phase_index = points[:, None] * freqs[None, :] % lon_points
    angles = phase_index.astype(jnp.float32) * (2.0 * math.pi / lon_points)
    factor = 1.0 / math.sqrt(lon_points)
    return jnp.concatenate([jnp.cos(angles) * factor, -jnp.sin(angles) * factor], axis=1).astype(jnp.bfloat16)

def apply_gain(spectrum, spec_gain, mode_count):
    spec_re = spectrum[..., :mode_count]
    spec_im = spectrum[..., mode_count:]
    gain_re = spec_gain[0][:, None, :]
    gain_im = spec_gain[1][:, None, :]
    return jnp.concatenate([gain_re * spec_re - gain_im * spec_im, gain_re * spec_im + gain_im * spec_re], axis=-1).astype(jnp.bfloat16)

def reference(field, land_mask, fold_partner, dw_kernel, norm_gain, w_in, w_out, spec_gain, mix_weight):
    wet_grid = land_mask.astype(field.dtype)
    masked = field * wet_grid[None]
    columns = (jnp.arange(LON + 6, dtype=jnp.int32) - 3) % LON
    lon_padded = jnp.take(masked, columns, axis=2)
    ghost_rows = jnp.take(masked[:, NLAT - 3:, :][:, ::-1, :], jnp.take(fold_partner, columns), axis=1 + 1)
    south_rows = jnp.zeros((C, 3, LON + 6), field.dtype)
    extended = jnp.concatenate([south_rows, lon_padded, ghost_rows], axis=1)
    fourier = dft_table(LON, M, 0, LON).astype(jnp.float32)
    w_in32 = w_in.astype(jnp.float32)
    w_out32 = w_out.astype(jnp.float32)
    mix32 = mix_weight.astype(jnp.float32)

    def row_block(block_index, result):
        offset = (block_index * RL).astype(jnp.int32)
        tile_rows = lax.dynamic_slice_in_dim(extended, offset, RL + 6, 1)
        depth = jnp.zeros((C, RL, LON), jnp.float32)
        for tap_row in range(7):
            for tap_col in range(7):
                weight_col = dw_kernel[:, tap_row, tap_col][:, None, None]
                depth = depth + weight_col * tile_rows[:, tap_row:tap_row + RL, tap_col:tap_col + LON].astype(jnp.float32)
        masked_rows = lax.dynamic_slice_in_dim(masked, offset, RL, 1).reshape(C, -1).astype(jnp.float32)
        wet_rows = lax.dynamic_slice_in_dim(wet_grid, offset, RL, 0).reshape(1, -1).astype(jnp.float32)
        flat = depth.reshape(C, -1)
        average = lax.optimization_barrier(jnp.mean(flat, axis=0, keepdims=True))
        centred = flat - average
        variance = lax.optimization_barrier(jnp.mean(centred * centred, axis=0, keepdims=True))
        normed = (centred * lax.rsqrt(variance + 1e-06) * norm_gain[:, None]).astype(jnp.bfloat16)
        pre_act = jnp.einsum('ch,cp->hp', w_in32, normed.astype(jnp.float32))
        hidden = jax.nn.gelu(pre_act, approximate=True).astype(jnp.bfloat16)
        branch = jnp.einsum('hc,hp->cp', w_out32, hidden.astype(jnp.float32))
        residual = (wet_rows * (masked_rows + branch)).astype(jnp.bfloat16)
        spectrum = jnp.dot(residual.reshape(C * RL, LON).astype(jnp.float32), fourier, preferred_element_type=jnp.float32)
        scaled = apply_gain(spectrum.reshape(C, RL, 2 * M), spec_gain, M)
        spatial = jnp.dot(scaled.reshape(C * RL, 2 * M).astype(jnp.float32), fourier.T, preferred_element_type=jnp.float32)
        spatial = spatial.astype(jnp.bfloat16).reshape(C, RL * LON)
        mixed = jnp.einsum('cd,cp->dp', mix32, spatial.astype(jnp.float32))
        output = (wet_rows * (residual.astype(jnp.float32) + mixed)).astype(jnp.bfloat16).reshape(C, RL, LON)
        return lax.dynamic_update_slice_in_dim(result, output, offset, 1)
    return lax.fori_loop(0, NLAT // RL, row_block, jnp.zeros(field.shape, jnp.bfloat16))
```

```python
import functools
import math

import jax
import jax.numpy as jnp
import numpy as np
from jax import lax
from jax.experimental import pallas as pl
from jax.experimental.pallas import tpu as pltpu
from jax.sharding import PartitionSpec as P

F32 = jnp.float32
BF16 = jnp.bfloat16
TAPS = 7
HALO = 3
LANES = 128


def dft_table(lon_points, mode_count):
    phase = np.arange(lon_points)[:, None] * np.arange(mode_count)[None, :] % lon_points
    angles = phase.astype(np.float32) * np.float32(2.0 * math.pi / lon_points)
    factor = np.float32(1.0 / math.sqrt(lon_points))
    angles = angles.astype(np.float64)
    table = np.concatenate([np.cos(angles), -np.sin(angles)], axis=1).astype(np.float32)
    return (table * factor).astype(BF16)


def kernel(
    sizes,
    field_ref, mask_ref, fold_ref, taps_ref, gain_ref, w_in_ref, w_out_ref, mix_ref, spec_hbm, table_hbm,
    out_ref,
    flat, ext, own, depth, res, by_rows, back, spatial,
    edge_mine, edge_left, edge_right, comb, comb_n, comb_s, rows_n, rows_s, top_all,
    spec_ref, table_ref,
    local_sem, edge_send, edge_recv, comb_send, comb_recv, rows_send, rows_recv,
    fold_send, fold_recv, out_send, out_recv, in_send, in_recv,
):
    channels, padded, rows, cols, lat_n, lon_n, modes = sizes
    lon_points = cols * lon_n
    per = rows // lon_n
    lat = lax.axis_index("lat")
    lon = lax.axis_index("lon")
    left = lax.rem(lon + lon_n - 1, lon_n)
    right = lax.rem(lon + 1, lon_n)
    chip = lon // 2
    core = lax.rem(lon, 2)
    chips = lon_n // 2

    def target(k):
        return lax.rem(chip + k // 2, chips) * 2 + lax.rem(core + lax.rem(k, 2), 2)

    def source(k):
        return lax.rem(chip + chips - k // 2, chips) * 2 + lax.rem(core + lax.rem(k, 2), 2)

    table_copy = pltpu.make_async_copy(table_hbm, table_ref, local_sem.at[0])
    spec_copy = pltpu.make_async_copy(spec_hbm, spec_ref, local_sem.at[1])
    table_copy.start()
    spec_copy.start()

    barrier = pltpu.get_barrier_semaphore()
    for k in range(1, lon_n):
        pl.semaphore_signal(barrier, inc=1, device_id={"lon": target(k)})

    @pl.when(lat > 0)
    def _():
        pl.semaphore_signal(barrier, inc=1, device_id={"lat": lat - 1})

    @pl.when(lat < lat_n - 1)
    def _():
        pl.semaphore_signal(barrier, inc=1, device_id={"lat": lat + 1})

    wet = mask_ref[...].astype(F32)

    @pl.loop(0, channels)
    def _(c):
        val = field_ref[c].astype(F32) * wet
        at = pl.multiple_of(c * rows, rows)
        flat[0, pl.ds(at, rows), :] = val[:, :LANES]
        flat[1, pl.ds(at, rows), :] = val[:, LANES:]

    tail = (padded - channels) * rows
    if tail:
        for h in range(2):
            flat[h, channels * rows :, :] = jnp.zeros((tail, LANES), F32)

    lane = lax.broadcasted_iota(jnp.int32, (padded, LANES), 1)
    pack = jnp.zeros((padded, LANES), F32)
    edge_mine[...] = pack.astype(BF16)
    for i in range(rows):
        lo = flat[0, pl.ds(i, padded, stride=rows), :]
        hi = flat[1, pl.ds(i, padded, stride=rows), :]
        own[i, :, :LANES] = lo.astype(BF16)
        own[i, :, LANES:] = hi.astype(BF16)
        ext[i + HALO, :, :LANES] = lo
        ext[i + HALO, :, LANES : 2 * LANES] = hi
        edge = jnp.where(lane < HALO, lo, jnp.where(lane >= LANES - HALO, hi, 0.0))
        if i:
            edge = pltpu.roll(edge, 8 * i, 1)
        edge_mine[...] = (edge_mine[...].astype(F32) + edge).astype(BF16)

    count = lon_n - 1 + jnp.where(lat > 0, 1, 0) + jnp.where(lat < lat_n - 1, 1, 0)
    pl.semaphore_wait(barrier, count)

    to_left = pltpu.make_async_remote_copy(
        edge_mine, edge_right, edge_send.at[0], edge_recv.at[0], device_id={"lon": left})
    to_right = pltpu.make_async_remote_copy(
        edge_mine, edge_left, edge_send.at[1], edge_recv.at[1], device_id={"lon": right})
    to_left.start()
    to_right.start()

    rows_down = pltpu.make_async_remote_copy(
        own.at[pl.ds(0, HALO)], rows_n, rows_send.at[0], rows_recv.at[0], device_id={"lat": lat - 1})
    rows_up = pltpu.make_async_remote_copy(
        own.at[pl.ds(rows - HALO, HALO)], rows_s, rows_send.at[1], rows_recv.at[1], device_id={"lat": lat + 1})
    comb_down = pltpu.make_async_remote_copy(
        comb, comb_n, comb_send.at[0], comb_recv.at[0], device_id={"lat": lat - 1})
    comb_up = pltpu.make_async_remote_copy(
        comb, comb_s, comb_send.at[1], comb_recv.at[1], device_id={"lat": lat + 1})

    def fold_copy(k):
        at = pl.multiple_of(lon * cols, LANES)
        return pltpu.make_async_remote_copy(
            own.at[pl.ds(rows - HALO, HALO)], top_all.at[:, :, pl.ds(at, cols)],
            fold_send.at[k - 1], fold_recv.at[k - 1], device_id={"lon": target(k)})

    @pl.when(lat > 0)
    def _():
        rows_down.start()

    @pl.when(lat < lat_n - 1)
    def _():
        rows_up.start()

    @pl.when(lat == lat_n - 1)
    def _():
        for k in range(lon_n - 1, 0, -1):
            fold_copy(k).start()
        top_all[:, :, pl.ds(pl.multiple_of(lon * cols, LANES), cols)] = own[rows - HALO :]

    to_left.wait()
    to_right.wait()
    both = jnp.where(lax.rem(lane, 8) < 4, edge_right[...].astype(F32), edge_left[...].astype(F32))
    comb[...] = both.astype(BF16)

    @pl.when(lat > 0)
    def _():
        comb_down.start()

    @pl.when(lat < lat_n - 1)
    def _():
        comb_up.start()

    def edges_of(packed, i):
        return pltpu.roll(packed, LANES - 8 * i, 1) if i else packed

    for i in range(rows):
        ext[i + HALO, :, 2 * LANES :] = edges_of(comb[...].astype(F32), i)

    def conv(out_rows):
        lo_e, hi_e = min(out_rows), max(out_rows) + TAPS

        @pl.loop(0, padded // 8)
        def _(group):
            at = pl.multiple_of(group * 8, 8)
            taps = taps_ref[pl.ds(at, 8), :]
            acc = {}
            for b in range(TAPS):
                weights = [
                    jnp.broadcast_to(taps[:, a * TAPS + b : a * TAPS + b + 1], (8, cols))
                    for a in range(TAPS)
                ]
                for e in range(lo_e, hi_e):
                    line = ext[e, pl.ds(at, 8), :]
                    if b != HALO:
                        line = pltpu.roll(line, (HALO - b) % (cols + LANES), 1)
                    line = line[:, :cols]
                    for a in range(TAPS):
                        i = e - a
                        if i in out_rows:
                            term = weights[a] * line
                            acc[i] = acc[i] + term if i in acc else term
            for i in out_rows:
                depth[i, pl.ds(at, 8), :] = acc[i]

    conv(list(range(HALO, rows - HALO)))

    @pl.when(lat > 0)
    def _():
        rows_down.wait_send()
        comb_down.wait_send()
        rows_up.wait_recv()
        comb_up.wait_recv()
        for r in range(HALO):
            ext[r, :, :cols] = rows_s[r].astype(F32)
            ext[r, :, cols:] = edges_of(comb_s[...].astype(F32), rows - HALO + r)

    @pl.when(lat == 0)
    def _():
        for r in range(HALO):
            ext[r] = jnp.zeros((padded, cols + LANES), F32)

    @pl.when(lat < lat_n - 1)
    def _():
        rows_up.wait_send()
        comb_up.wait_send()
        rows_down.wait_recv()
        comb_down.wait_recv()
        for r in range(HALO):
            ext[rows + HALO + r, :, :cols] = rows_n[r].astype(F32)
            ext[rows + HALO + r, :, cols:] = edges_of(comb_n[...].astype(F32), r)

    @pl.when(lat == lat_n - 1)
    def _():
        for k in range(lon_n - 1, 0, -1):
            fold_copy(k).wait()
        point = lax.broadcasted_iota(jnp.int32, (lon_points, cols + LANES), 0)
        pick = jnp.where(point == fold_ref[...], 1.0, 0.0).astype(BF16)
        for r in range(HALO):
            ext[rows + HALO + r] = jnp.dot(top_all[HALO - 1 - r], pick, preferred_element_type=F32)

    conv(list(range(HALO)))
    conv(list(range(rows - HALO, rows)))

    inside = lax.broadcasted_iota(jnp.int32, (padded, cols), 0) < channels

    def send_row(t):
        k = lon_n - 1 - t // per
        row = target(k) * per + lax.rem(t, per)
        return pltpu.make_async_remote_copy(
            res.at[row], by_rows.at[lax.rem(t, per), :, pl.ds(pl.multiple_of(lon * cols, LANES), cols)],
            out_send.at[t], out_recv.at[t], device_id={"lon": target(k)})

    @pl.loop(0, rows)
    def _(t):
        k = lon_n - 1 - t // per
        row = target(k) * per + lax.rem(t, per)
        x = depth[row]
        mean = jnp.sum(x, axis=0, keepdims=True) * (1.0 / channels)
        centred = jnp.where(inside, x - mean, 0.0)
        var = jnp.sum(centred * centred, axis=0, keepdims=True) * (1.0 / channels)
        normed = (centred * lax.rsqrt(var + 1e-06) * gain_ref[...]).astype(BF16)
        pre = jnp.dot(w_in_ref[...], normed, preferred_element_type=F32)
        hidden = jax.nn.gelu(pre, approximate=True).astype(BF16)
        branch = jnp.dot(w_out_ref[...], hidden, preferred_element_type=F32)
        wet_row = mask_ref[pl.ds(row, 1), :].astype(F32)
        val = (wet_row * (own[row].astype(F32) + branch)).astype(BF16)
        res[row] = val

        @pl.when(t < (lon_n - 1) * per)
        def _():
            send_row(t).start()

        @pl.when(t >= (lon_n - 1) * per)
        def _():
            by_rows[lax.rem(t, per), :, pl.ds(pl.multiple_of(lon * cols, LANES), cols)] = val

    table_copy.wait()
    spec_copy.wait()

    def send_back(r, k):
        q = target(k)
        s = (lon_n - 1 - k) * per + r
        return pltpu.make_async_remote_copy(
            back.at[r, :, pl.ds(pl.multiple_of(q * cols, LANES), cols)], spatial.at[lon * per + r],
            in_send.at[s], in_recv.at[s], device_id={"lon": q})

    @pl.loop(0, per)
    def _(r):
        for kk in range(lon_n - 1):
            send_row(kk * per + r).wait_recv()
        spectrum = jnp.dot(by_rows[r], table_ref[...], preferred_element_type=F32)
        s_re = spectrum[:, :modes]
        s_im = spectrum[:, modes:]
        g_re = spec_ref[0]
        g_im = spec_ref[1]
        scaled = jnp.concatenate(
            [(g_re * s_re - g_im * s_im).astype(BF16), (g_re * s_im + g_im * s_re).astype(BF16)], axis=1)
        back[r] = lax.dot_general(
            scaled, table_ref[...], (((1,), (1,)), ((), ())), preferred_element_type=F32).astype(BF16)
        for k in range(lon_n - 1, 0, -1):
            send_back(r, k).start()
        spatial[lon * per + r] = back[r, :, pl.ds(pl.multiple_of(lon * cols, LANES), cols)]

    @pl.loop(0, rows)
    def _(t):
        k = t // per
        row = source(k) * per + lax.rem(t, per)

        @pl.when(t >= per)
        def _():
            send_back(lax.rem(t, per), k).wait_recv()

        mixed = jnp.dot(mix_ref[...], spatial[row], preferred_element_type=F32)
        wet_row = mask_ref[pl.ds(row, 1), :].astype(F32)
        val = wet_row * (res[row].astype(F32) + mixed)
        flat[0, pl.ds(row, padded, stride=rows), :] = val[:, :LANES]
        flat[1, pl.ds(row, padded, stride=rows), :] = val[:, LANES:]

    @pl.loop(0, channels)
    def _(c):
        at = pl.multiple_of(c * rows, rows)
        out_ref[c, :, :LANES] = flat[0, pl.ds(at, rows), :].astype(BF16)
        out_ref[c, :, LANES:] = flat[1, pl.ds(at, rows), :].astype(BF16)

    @pl.loop(0, (lon_n - 1) * per)
    def _(t):
        send_row(t).wait_send()
        send_back(lax.rem(t, per), lon_n - 1 - t // per).wait_send()


def local(lat_n, lon_n, field, land_mask, fold_partner, dw_kernel, norm_gain, w_in, w_out, spec_gain, mix_weight):
    channels, rows, cols = field.shape
    modes = spec_gain.shape[2]
    hid = w_in.shape[1]
    lon_points = cols * lon_n
    padded = -(-channels // 16) * 16
    hid_pad = -(-hid // 16) * 16
    extra = padded - channels
    table = jnp.asarray(dft_table(lon_points, modes))
    lane = jnp.arange(cols + LANES, dtype=jnp.int32)
    column = jnp.where(lane < cols + HALO, lane, lane - (cols + LANES))
    fold = (fold_partner[0] - (lax.axis_index("lon") * cols + column)) % lon_points
    taps = jnp.pad(dw_kernel.reshape(channels, -1), ((0, extra), (0, LANES - TAPS * TAPS)))
    gain = jnp.pad(norm_gain, (0, extra))[:, None]
    w_in_t = jnp.pad(w_in.T, ((0, hid_pad - hid), (0, extra)))
    w_out_t = jnp.pad(w_out.T, ((0, extra), (0, hid_pad - hid)))
    mix_t = jnp.pad(mix_weight.T, ((0, extra), (0, extra)))
    spec = jnp.pad(spec_gain, ((0, 0), (0, extra), (0, 0)))
    per = rows // lon_n
    sizes = (channels, padded, rows, cols, lat_n, lon_n, modes)
    vmem = pl.BlockSpec(memory_space=pltpu.VMEM)
    hbm = pl.BlockSpec(memory_space=pl.ANY)
    dma = pltpu.SemaphoreType.DMA
    peers = lon_n - 1
    return pl.pallas_call(
        functools.partial(kernel, sizes),
        out_shape=jax.ShapeDtypeStruct(field.shape, BF16),
        in_specs=[vmem] * 8 + [hbm] * 2,
        out_specs=vmem,
        scratch_shapes=[
            pltpu.VMEM((2, padded * rows, LANES), F32),
            pltpu.VMEM((rows + 2 * HALO, padded, cols + LANES), F32),
            pltpu.VMEM((rows, padded, cols), BF16),
            pltpu.VMEM((rows, padded, cols), F32),
            pltpu.VMEM((rows, padded, cols), BF16),
            pltpu.VMEM((per, padded, lon_points), BF16),
            pltpu.VMEM((per, padded, lon_points), BF16),
            pltpu.VMEM((rows, padded, cols), BF16),
            *[pltpu.VMEM((padded, LANES), BF16)] * 6,
            *[pltpu.VMEM((HALO, padded, cols), BF16)] * 2,
            pltpu.VMEM((HALO, padded, lon_points), BF16),
            pltpu.VMEM(spec.shape, F32),
            pltpu.VMEM(table.shape, BF16),
            *[dma((2,))] * 7,
            *[dma((peers,))] * 2,
            *[dma((peers * per,))] * 4,
        ],
        compiler_params=pltpu.CompilerParams(
            collective_id=0, has_side_effects=True, vmem_limit_bytes=62 * 1024 * 1024),
        name="block",
    )(field, land_mask, fold[None, :], taps, gain, w_in_t, w_out_t, mix_t, spec, table)


def solution(mesh):
    placed = (P(None, "lat", "lon"), P("lat", "lon"), P(), P(), P(), P(), P(), P(), P())
    return jax.shard_map(
        functools.partial(local, mesh.shape["lat"], mesh.shape["lon"]),
        mesh=mesh, in_specs=placed, out_specs=P(None, "lat", "lon"), check_vma=False,
    )
```

```python
import functools
import math

import jax
import jax.numpy as jnp
import numpy as np
from jax import lax
from jax.experimental import pallas as pl
from jax.experimental.pallas import tpu as pltpu
from jax.sharding import PartitionSpec as P

F32 = jnp.float32
BF16 = jnp.bfloat16
TAPS = 7
HALO = 3
LANES = 128


def dft_table(lon_points, mode_count):
    phase = np.arange(lon_points)[:, None] * np.arange(mode_count)[None, :] % lon_points
    angles = phase.astype(np.float32) * np.float32(2.0 * math.pi / lon_points)
    factor = np.float32(1.0 / math.sqrt(lon_points))
    angles = angles.astype(np.float64)
    table = np.concatenate([np.cos(angles), -np.sin(angles)], axis=1).astype(np.float32)
    return (table * factor).astype(BF16)


def kernel(
    sizes,
    field_ref, mask_ref, fold_ref, taps_ref, gain_ref, w_in_ref, w_out_ref, mix_ref, spec_hbm, table_hbm,
    out_ref,
    flat, ext, own, depth, res, by_rows, back, spatial,
    edge_mine, edge_left, edge_right, comb, comb_n, comb_s, rows_n, rows_s, top_all,
    spec_ref, table_ref, wide_taps, w_in_t, w_out_t, mix_t, gain_col,
    local_sem, edge_send, edge_recv, comb_send, comb_recv, rows_send, rows_recv,
    fold_send, fold_recv, out_send, out_recv, in_send, in_recv,
):
    channels, padded, rows, cols, lat_n, lon_n, modes = sizes
    lon_points = cols * lon_n
    per = rows // lon_n
    lat = lax.axis_index("lat")
    lon = lax.axis_index("lon")
    left = lax.rem(lon + lon_n - 1, lon_n)
    right = lax.rem(lon + 1, lon_n)
    chip = lon // 2
    core = lax.rem(lon, 2)
    chips = lon_n // 2

    def target(k):
        return lax.rem(chip + k // 2, chips) * 2 + lax.rem(core + lax.rem(k, 2), 2)

    def source(k):
        return lax.rem(chip + chips - k // 2, chips) * 2 + lax.rem(core + lax.rem(k, 2), 2)

    table_copy = pltpu.make_async_copy(table_hbm, table_ref, local_sem.at[0])
    spec_copy = pltpu.make_async_copy(spec_hbm, spec_ref, local_sem.at[1])
    table_copy.start()
    spec_copy.start()

    barrier = pltpu.get_barrier_semaphore()
    for k in range(1, lon_n):
        pl.semaphore_signal(barrier, inc=1, device_id={"lon": target(k)})

    @pl.when(lat > 0)
    def _():
        pl.semaphore_signal(barrier, inc=1, device_id={"lat": lat - 1})

    @pl.when(lat < lat_n - 1)
    def _():
        pl.semaphore_signal(barrier, inc=1, device_id={"lat": lat + 1})

    wet = mask_ref[...].astype(F32)

    @pl.loop(0, channels)
    def _(c):
        val = field_ref[c].astype(F32) * wet
        at = pl.multiple_of(c * rows, rows)
        flat[0, pl.ds(at, rows), :] = val[:, :LANES]
        flat[1, pl.ds(at, rows), :] = val[:, LANES:]

    tail = (padded - channels) * rows
    if tail:
        for h in range(2):
            flat[h, channels * rows :, :] = jnp.zeros((tail, LANES), F32)

    lane = lax.broadcasted_iota(jnp.int32, (padded, LANES), 1)
    pack = jnp.zeros((padded, LANES), F32)
    edge_mine[...] = pack.astype(BF16)
    for i in range(rows):
        lo = flat[0, pl.ds(i, padded, stride=rows), :]
        hi = flat[1, pl.ds(i, padded, stride=rows), :]
        own[i, :, :LANES] = lo.astype(BF16)
        own[i, :, LANES:] = hi.astype(BF16)
        ext[i + HALO, :, :LANES] = lo
        ext[i + HALO, :, LANES : 2 * LANES] = hi
        edge = jnp.where(lane < HALO, lo, jnp.where(lane >= LANES - HALO, hi, 0.0))
        if i:
            edge = pltpu.roll(edge, 8 * i, 1)
        edge_mine[...] = (edge_mine[...].astype(F32) + edge).astype(BF16)

    count = lon_n - 1 + jnp.where(lat > 0, 1, 0) + jnp.where(lat < lat_n - 1, 1, 0)
    pl.semaphore_wait(barrier, count)

    to_left = pltpu.make_async_remote_copy(
        edge_mine, edge_right, edge_send.at[0], edge_recv.at[0], device_id={"lon": left})
    to_right = pltpu.make_async_remote_copy(
        edge_mine, edge_left, edge_send.at[1], edge_recv.at[1], device_id={"lon": right})
    to_left.start()
    to_right.start()

    rows_down = pltpu.make_async_remote_copy(
        own.at[pl.ds(0, HALO)], rows_n, rows_send.at[0], rows_recv.at[0], device_id={"lat": lat - 1})
    rows_up = pltpu.make_async_remote_copy(
        own.at[pl.ds(rows - HALO, HALO)], rows_s, rows_send.at[1], rows_recv.at[1], device_id={"lat": lat + 1})
    comb_down = pltpu.make_async_remote_copy(
        comb, comb_n, comb_send.at[0], comb_recv.at[0], device_id={"lat": lat - 1})
    comb_up = pltpu.make_async_remote_copy(
        comb, comb_s, comb_send.at[1], comb_recv.at[1], device_id={"lat": lat + 1})

    def fold_copy(k):
        at = pl.multiple_of(lon * cols, LANES)
        return pltpu.make_async_remote_copy(
            own.at[pl.ds(rows - HALO, HALO)], top_all.at[:, :, pl.ds(at, cols)],
            fold_send.at[k - 1], fold_recv.at[k - 1], device_id={"lon": target(k)})

    @pl.when(lat > 0)
    def _():
        rows_down.start()

    @pl.when(lat < lat_n - 1)
    def _():
        rows_up.start()

    @pl.when(lat == lat_n - 1)
    def _():
        for k in range(lon_n - 1, 0, -1):
            fold_copy(k).start()
        top_all[:, :, pl.ds(pl.multiple_of(lon * cols, LANES), cols)] = own[rows - HALO :]

    wide_taps[:, padded - 16 :, :] = jnp.zeros((TAPS * TAPS, 16, LANES), F32)
    for t in range(TAPS * TAPS):
        wide_taps[t, :channels, :] = jnp.broadcast_to(taps_ref[:, t : t + 1], (channels, LANES))

    def turned(ref, target_ref):
        n, m = ref.shape
        up = [-(-d // LANES) * LANES for d in (n, m)]
        full = jnp.concatenate([ref[...].astype(F32), jnp.zeros((n, up[1] - m), F32)], axis=1)
        full = jnp.concatenate([full, jnp.zeros((up[0] - n, up[1]), F32)], axis=0)
        target_ref[...] = full.T[: target_ref.shape[0], : target_ref.shape[1]].astype(BF16)

    turned(w_in_ref, w_in_t)
    turned(w_out_ref, w_out_t)
    turned(mix_ref, mix_t)
    diagonal = lax.broadcasted_iota(jnp.int32, (padded, channels), 0) == lax.broadcasted_iota(
        jnp.int32, (padded, channels), 1)
    gain_col[...] = jnp.broadcast_to(
        jnp.sum(jnp.where(diagonal, gain_ref[...], 0.0), axis=1, keepdims=True), (padded, LANES))
    back[:, padded - 16 :, :] = jnp.zeros((per, 16, lon_points), BF16)

    to_left.wait()
    to_right.wait()
    both = jnp.where(lax.rem(lane, 8) < 4, edge_right[...].astype(F32), edge_left[...].astype(F32))
    comb[...] = both.astype(BF16)

    @pl.when(lat > 0)
    def _():
        comb_down.start()

    @pl.when(lat < lat_n - 1)
    def _():
        comb_up.start()

    def edges_of(packed, i):
        return pltpu.roll(packed, LANES - 8 * i, 1) if i else packed

    for i in range(rows):
        ext[i + HALO, :, 2 * LANES :] = edges_of(comb[...].astype(F32), i)

    def conv(out_rows):
        lines = sorted({i + a for i in out_rows for a in range(TAPS)})

        @pl.loop(0, padded // 16)
        def _(group):
            for half in range(2):
                at = pl.multiple_of(group * 16 + half * 8, 8)
                acc = {}
                for b in range(TAPS):
                    weights = [wide_taps[a * TAPS + b, pl.ds(at, 8), :] for a in range(TAPS)]
                    for e in lines:
                        line = ext[e, pl.ds(at, 8), :]
                        if b != HALO:
                            line = pltpu.roll(line, (HALO - b) % (cols + LANES), 1)
                        for a in range(TAPS):
                            i = e - a
                            if i in out_rows:
                                for h in range(cols // LANES):
                                    term = weights[a] * line[:, h * LANES : (h + 1) * LANES]
                                    acc[i, h] = acc[i, h] + term if (i, h) in acc else term
                for (i, h), total in acc.items():
                    depth[i, pl.ds(at, 8), h * LANES : (h + 1) * LANES] = total

    def await_halo():
        @pl.when(lat > 0)
        def _():
            rows_down.wait_send()
            comb_down.wait_send()
            rows_up.wait_recv()
            comb_up.wait_recv()
            for r in range(HALO):
                ext[r, :, :cols] = rows_s[r].astype(F32)
                ext[r, :, cols:] = edges_of(comb_s[...].astype(F32), rows - HALO + r)

        @pl.when(lat == 0)
        def _():
            for r in range(HALO):
                ext[r] = jnp.zeros((padded, cols + LANES), F32)

        @pl.when(lat < lat_n - 1)
        def _():
            rows_up.wait_send()
            comb_up.wait_send()
            rows_down.wait_recv()
            comb_down.wait_recv()
            for r in range(HALO):
                ext[rows + HALO + r, :, :cols] = rows_n[r].astype(F32)
                ext[rows + HALO + r, :, cols:] = edges_of(comb_n[...].astype(F32), r)

        @pl.when(lat == lat_n - 1)
        def _():
            for k in range(lon_n - 1, 0, -1):
                fold_copy(k).wait()
            point = lax.broadcasted_iota(jnp.int32, (lon_points, cols + LANES), 0)
            at = lax.broadcasted_iota(jnp.int32, (1, cols + LANES), 1)
            at = jnp.where(at < cols + HALO, at, at - (cols + LANES)) + lon * cols
            mate = fold_ref[:, :1] - at
            mate = jnp.where(mate < 0, mate + lon_points, mate)
            mate = jnp.where(mate < 0, mate + lon_points, mate)
            mate = jnp.where(mate >= lon_points, mate - lon_points, mate)
            pick = jnp.where(point == mate, 1.0, 0.0).astype(BF16)
            for r in range(HALO):
                ext[rows + HALO + r] = jnp.dot(top_all[HALO - 1 - r], pick, preferred_element_type=F32)

    here = pl.ds(pl.multiple_of(lon * cols, LANES), cols)

    def row_at(chunk, q):
        return lax.rem(chunk * lon_n + q + HALO, rows)

    def send_row(chunk, k):
        s = chunk * (lon_n - 1) + lon_n - 1 - k
        return pltpu.make_async_remote_copy(
            res.at[row_at(chunk, target(k))], by_rows.at[chunk, :, here],
            out_send.at[s], out_recv.at[s], device_id={"lon": target(k)})

    def send_back(chunk, k):
        q = target(k)
        s = chunk * (lon_n - 1) + lon_n - 1 - k
        return pltpu.make_async_remote_copy(
            back.at[chunk, :, pl.ds(pl.multiple_of(q * cols, LANES), cols)], spatial.at[chunk * lon_n + lon],
            in_send.at[s], in_recv.at[s], device_id={"lon": q})

    inside = lax.broadcasted_iota(jnp.int32, (padded, 2 * cols), 0) < channels

    def mix_rows(chunk):
        @pl.loop(0, lon_n // 2)
        def _(pair):
            k = lon_n - 1 - 2 * pair
            one, two = row_at(chunk, target(k)), row_at(chunk, target(k - 1))
            x = jnp.concatenate([depth[one], depth[two]], axis=1)
            mean = jnp.sum(x, axis=0, keepdims=True) * (1.0 / channels)
            centred = jnp.where(inside, x - mean, 0.0)
            var = jnp.sum(centred * centred, axis=0, keepdims=True) * (1.0 / channels)
            normed = (centred * lax.rsqrt(var + 1e-06) * gain_col[:, :1]).astype(BF16)
            pre = jnp.dot(w_in_t[...], normed, preferred_element_type=F32)
            hidden = jax.nn.gelu(pre, approximate=True).astype(BF16)
            branch = jnp.dot(w_out_t[...], hidden, preferred_element_type=F32)
            for n, row in enumerate((one, two)):
                wet_row = mask_ref[pl.ds(row, 1), :].astype(F32)
                part = branch[:, n * cols : (n + 1) * cols]
                res[row] = (wet_row * (own[row].astype(F32) + part)).astype(BF16)
            send_row(chunk, k).start()

            @pl.when(pair < lon_n // 2 - 1)
            def _():
                send_row(chunk, k - 1).start()

            @pl.when(pair == lon_n // 2 - 1)
            def _():
                by_rows[chunk, :, here] = res[two]

    def spectral(chunk):
        for k in range(lon_n - 1, 0, -1):
            send_row(chunk, k).wait_recv()
        spectrum = jnp.dot(by_rows[chunk], table_ref[...], preferred_element_type=F32)
        s_re = spectrum[:channels, :modes]
        s_im = spectrum[:channels, modes:]
        g_re = spec_ref[0]
        g_im = spec_ref[1]
        scaled = jnp.concatenate(
            [(g_re * s_re - g_im * s_im).astype(BF16), (g_re * s_im + g_im * s_re).astype(BF16)], axis=1)
        back[chunk, :channels] = lax.dot_general(
            scaled, table_ref[...], (((1,), (1,)), ((), ())), preferred_element_type=F32).astype(BF16)
        for k in range(lon_n - 1, 0, -1):
            send_back(chunk, k).start()
        spatial[chunk * lon_n + lon] = back[chunk, :, here]

    def finish(chunk):
        @pl.loop(0, lon_n)
        def _(k):
            @pl.when(k > 0)
            def _():
                send_back(chunk, k).wait_recv()

            pos = source(k)
            row = row_at(chunk, pos)
            mixed = jnp.dot(mix_t[...], spatial[chunk * lon_n + pos], preferred_element_type=F32)
            wet_row = mask_ref[pl.ds(row, 1), :].astype(F32)
            val = wet_row * (res[row].astype(F32) + mixed)
            flat[0, pl.ds(row, padded, stride=rows), :] = val[:, :LANES]
            flat[1, pl.ds(row, padded, stride=rows), :] = val[:, LANES:]

    halo_done = False
    for chunk in range(per):
        out_rows = [(chunk * lon_n + q + HALO) % rows for q in range(lon_n)]
        if not halo_done and (min(out_rows) < HALO or max(out_rows) >= rows - HALO):
            await_halo()
            halo_done = True
        conv(out_rows)
        mix_rows(chunk)
        if chunk == 1:
            table_copy.wait()
            spec_copy.wait()
        if chunk >= 1:
            spectral(chunk - 1)
    if per == 1:
        table_copy.wait()
        spec_copy.wait()
    for chunk in range(per - 2):
        finish(chunk)
    spectral(per - 1)
    for chunk in range(max(per - 2, 0), per):
        finish(chunk)

    @pl.loop(0, channels)
    def _(c):
        at = pl.multiple_of(c * rows, rows)
        out_ref[c, :, :LANES] = flat[0, pl.ds(at, rows), :].astype(BF16)
        out_ref[c, :, LANES:] = flat[1, pl.ds(at, rows), :].astype(BF16)

    for chunk in range(per):
        for k in range(lon_n - 1, 0, -1):
            send_row(chunk, k).wait_send()
            send_back(chunk, k).wait_send()


def local(lat_n, lon_n, field, land_mask, fold_partner, dw_kernel, norm_gain, w_in, w_out, spec_gain, mix_weight):
    channels, rows, cols = field.shape
    modes = spec_gain.shape[2]
    hid = w_in.shape[1]
    lon_points = cols * lon_n
    padded = -(-channels // 16) * 16
    hid_up = -(-hid // 16) * 16
    table = jnp.asarray(dft_table(lon_points, modes))
    taps = dw_kernel.reshape(channels, -1)
    per = rows // lon_n
    sizes = (channels, padded, rows, cols, lat_n, lon_n, modes)
    vmem = pl.BlockSpec(memory_space=pltpu.VMEM)
    hbm = pl.BlockSpec(memory_space=pl.ANY)
    dma = pltpu.SemaphoreType.DMA
    peers = lon_n - 1
    return pl.pallas_call(
        functools.partial(kernel, sizes),
        out_shape=jax.ShapeDtypeStruct(field.shape, BF16),
        in_specs=[vmem] * 8 + [hbm] * 2,
        out_specs=vmem,
        scratch_shapes=[
            pltpu.VMEM((2, padded * rows, LANES), F32),
            pltpu.VMEM((rows + 2 * HALO, padded, cols + LANES), F32),
            pltpu.VMEM((rows, padded, cols), BF16),
            pltpu.VMEM((rows, padded, cols), F32),
            pltpu.VMEM((rows, padded, cols), BF16),
            pltpu.VMEM((per, padded, lon_points), BF16),
            pltpu.VMEM((per, padded, lon_points), BF16),
            pltpu.VMEM((rows, padded, cols), BF16),
            *[pltpu.VMEM((padded, LANES), BF16)] * 6,
            *[pltpu.VMEM((HALO, padded, cols), BF16)] * 2,
            pltpu.VMEM((HALO, padded, lon_points), BF16),
            pltpu.VMEM(spec_gain.shape, F32),
            pltpu.VMEM(table.shape, BF16),
            pltpu.VMEM((TAPS * TAPS, padded, LANES), F32),
            pltpu.VMEM((hid_up, padded), BF16),
            pltpu.VMEM((padded, hid_up), BF16),
            pltpu.VMEM((padded, padded), BF16),
            pltpu.VMEM((padded, LANES), F32),
            *[dma((2,))] * 7,
            *[dma((peers,))] * 2,
            *[dma((peers * per,))] * 4,
        ],
        compiler_params=pltpu.CompilerParams(
            collective_id=0, has_side_effects=True, vmem_limit_bytes=62 * 1024 * 1024),
        name="block",
    )(field, land_mask, fold_partner[None, :], taps, norm_gain[None, :], w_in, w_out, mix_weight, spec_gain, table)


def solution(mesh):
    placed = (P(None, "lat", "lon"), P("lat", "lon"), P(), P(), P(), P(), P(), P(), P())
    return jax.shard_map(
        functools.partial(local, mesh.shape["lat"], mesh.shape["lon"]),
        mesh=mesh, in_specs=placed, out_specs=P(None, "lat", "lon"), check_vma=False,
    )
```

```python
import functools
import math

import jax
import jax.numpy as jnp
import numpy as np
from jax import lax
from jax.experimental import pallas as pl
from jax.experimental.pallas import tpu as pltpu
from jax.sharding import PartitionSpec as P

F32 = jnp.float32
BF16 = jnp.bfloat16
TAPS = 7
HALO = 3
LANES = 128


def dft_table(lon_points, mode_count):
    phase = np.arange(lon_points)[:, None] * np.arange(mode_count)[None, :] % lon_points
    angles = phase.astype(np.float32) * np.float32(2.0 * math.pi / lon_points)
    factor = np.float32(1.0 / math.sqrt(lon_points))
    angles = angles.astype(np.float64)
    table = np.concatenate([np.cos(angles), -np.sin(angles)], axis=1).astype(np.float32)
    return (table * factor).astype(BF16)


def kernel(
    sizes,
    field_ref, mask_ref, fold_ref, taps_ref, gain_ref, w_in_ref, w_out_ref, mix_ref, spec_hbm, table_hbm,
    out_ref,
    flat, ext, own, depth, res, by_rows, back, spatial,
    edge_mine, edge_left, edge_right, comb, comb_n, comb_s, rows_n, rows_s, top_all,
    spec_ref, table_ref, wide_taps, w_in_t, w_out_t, mix_t, gain_col,
    local_sem, edge_send, edge_recv, comb_send, comb_recv, rows_send, rows_recv,
    fold_send, fold_recv, out_send, out_recv, in_send, in_recv,
):
    channels, padded, rows, cols, lat_n, lon_n, modes = sizes
    lon_points = cols * lon_n
    per = rows // lon_n
    lat = lax.axis_index("lat")
    lon = lax.axis_index("lon")
    left = lax.rem(lon + lon_n - 1, lon_n)
    right = lax.rem(lon + 1, lon_n)
    chip = lon // 2
    core = lax.rem(lon, 2)
    chips = lon_n // 2

    def target(k):
        return lax.rem(chip + k // 2, chips) * 2 + lax.rem(core + lax.rem(k, 2), 2)

    def source(k):
        return lax.rem(chip + chips - k // 2, chips) * 2 + lax.rem(core + lax.rem(k, 2), 2)

    table_copy = pltpu.make_async_copy(table_hbm, table_ref, local_sem.at[0])
    spec_copy = pltpu.make_async_copy(spec_hbm, spec_ref, local_sem.at[1])
    table_copy.start()
    spec_copy.start()

    barrier = pltpu.get_barrier_semaphore()
    for k in range(1, lon_n):
        pl.semaphore_signal(barrier, inc=1, device_id={"lon": target(k)})

    @pl.when(lat > 0)
    def _():
        pl.semaphore_signal(barrier, inc=1, device_id={"lat": lat - 1})

    @pl.when(lat < lat_n - 1)
    def _():
        pl.semaphore_signal(barrier, inc=1, device_id={"lat": lat + 1})

    wet = mask_ref[...].astype(F32)

    @pl.loop(0, channels)
    def _(c):
        val = field_ref[c].astype(F32) * wet
        at = pl.multiple_of(c * rows, rows)
        flat[0, pl.ds(at, rows), :] = val[:, :LANES]
        flat[1, pl.ds(at, rows), :] = val[:, LANES:]

    tail = (padded - channels) * rows
    if tail:
        for h in range(2):
            flat[h, channels * rows :, :] = jnp.zeros((tail, LANES), F32)

    lane = lax.broadcasted_iota(jnp.int32, (padded, LANES), 1)
    pack = jnp.zeros((padded, LANES), F32)
    edge_mine[...] = pack.astype(BF16)
    for i in range(rows):
        lo = flat[0, pl.ds(i, padded, stride=rows), :]
        hi = flat[1, pl.ds(i, padded, stride=rows), :]
        own[i, :, :LANES] = lo.astype(BF16)
        own[i, :, LANES:] = hi.astype(BF16)
        ext[i + HALO, :, :LANES] = lo
        ext[i + HALO, :, LANES : 2 * LANES] = hi
        edge = jnp.where(lane < HALO, lo, jnp.where(lane >= LANES - HALO, hi, 0.0))
        if i:
            edge = pltpu.roll(edge, 8 * i, 1)
        edge_mine[...] = (edge_mine[...].astype(F32) + edge).astype(BF16)

    count = lon_n - 1 + jnp.where(lat > 0, 1, 0) + jnp.where(lat < lat_n - 1, 1, 0)
    pl.semaphore_wait(barrier, count)

    to_left = pltpu.make_async_remote_copy(
        edge_mine, edge_right, edge_send.at[0], edge_recv.at[0], device_id={"lon": left})
    to_right = pltpu.make_async_remote_copy(
        edge_mine, edge_left, edge_send.at[1], edge_recv.at[1], device_id={"lon": right})
    to_left.start()
    to_right.start()

    rows_down = pltpu.make_async_remote_copy(
        own.at[pl.ds(0, HALO)], rows_n, rows_send.at[0], rows_recv.at[0], device_id={"lat": lat - 1})
    rows_up = pltpu.make_async_remote_copy(
        own.at[pl.ds(rows - HALO, HALO)], rows_s, rows_send.at[1], rows_recv.at[1], device_id={"lat": lat + 1})
    comb_down = pltpu.make_async_remote_copy(
        comb, comb_n, comb_send.at[0], comb_recv.at[0], device_id={"lat": lat - 1})
    comb_up = pltpu.make_async_remote_copy(
        comb, comb_s, comb_send.at[1], comb_recv.at[1], device_id={"lat": lat + 1})

    def fold_copy(k):
        at = pl.multiple_of(lon * cols, LANES)
        return pltpu.make_async_remote_copy(
            own.at[pl.ds(rows - HALO, HALO)], top_all.at[:, :, pl.ds(at, cols)],
            fold_send.at[k - 1], fold_recv.at[k - 1], device_id={"lon": target(k)})

    @pl.when(lat > 0)
    def _():
        rows_down.start()

    @pl.when(lat < lat_n - 1)
    def _():
        rows_up.start()

    @pl.when(lat == lat_n - 1)
    def _():
        for k in range(lon_n - 1, 0, -1):
            fold_copy(k).start()
        top_all[:, :, pl.ds(pl.multiple_of(lon * cols, LANES), cols)] = own[rows - HALO :]

    wide_taps[:, padded - 16 :, :] = jnp.zeros((TAPS * TAPS, 16, LANES), F32)
    chan_up = -(-channels // LANES) * LANES
    for a in range(TAPS):
        line = jnp.concatenate([taps_ref[a], jnp.zeros((TAPS, chan_up - channels), F32)], axis=1)
        line = jnp.concatenate([line, jnp.zeros((LANES - TAPS, chan_up), F32)], axis=0).T
        for b in range(TAPS):
            wide_taps[a * TAPS + b, :channels, :] = jnp.broadcast_to(line[:channels, b : b + 1], (channels, LANES))

    def turned(ref, target_ref):
        n, m = ref.shape
        up = [-(-d // LANES) * LANES for d in (n, m)]
        full = jnp.concatenate([ref[...].astype(F32), jnp.zeros((n, up[1] - m), F32)], axis=1)
        full = jnp.concatenate([full, jnp.zeros((up[0] - n, up[1]), F32)], axis=0)
        target_ref[...] = full.T[: target_ref.shape[0], : target_ref.shape[1]].astype(BF16)

    turned(w_in_ref, w_in_t)
    hid = w_out_ref.shape[1]
    w_out_t[...] = jnp.zeros(w_out_t.shape, BF16)
    w_out_t[:channels, :hid] = w_out_ref[...]
    turned(mix_ref, mix_t)
    diagonal = lax.broadcasted_iota(jnp.int32, (padded, channels), 0) == lax.broadcasted_iota(
        jnp.int32, (padded, channels), 1)
    gain_col[...] = jnp.broadcast_to(
        jnp.sum(jnp.where(diagonal, gain_ref[...], 0.0), axis=1, keepdims=True), (padded, LANES))
    back[:, padded - 16 :, :] = jnp.zeros((per, 16, lon_points), BF16)

    to_left.wait()
    to_right.wait()
    both = jnp.where(lax.rem(lane, 8) < 4, edge_right[...].astype(F32), edge_left[...].astype(F32))
    comb[...] = both.astype(BF16)

    @pl.when(lat > 0)
    def _():
        comb_down.start()

    @pl.when(lat < lat_n - 1)
    def _():
        comb_up.start()

    def edges_of(packed, i):
        return pltpu.roll(packed, LANES - 8 * i, 1) if i else packed

    for i in range(rows):
        ext[i + HALO, :, 2 * LANES :] = edges_of(comb[...].astype(F32), i)

    def conv(out_rows):
        lines = sorted({i + a for i in out_rows for a in range(TAPS)})

        @pl.loop(0, padded // 16)
        def _(group):
            for half in range(2):
                at = pl.multiple_of(group * 16 + half * 8, 8)
                acc = {}
                for b in range(TAPS):
                    weights = [wide_taps[a * TAPS + b, pl.ds(at, 8), :] for a in range(TAPS)]
                    for e in lines:
                        line = ext[e, pl.ds(at, 8), :]
                        if b != HALO:
                            line = pltpu.roll(line, (HALO - b) % (cols + LANES), 1)
                        for a in range(TAPS):
                            i = e - a
                            if i in out_rows:
                                for h in range(cols // LANES):
                                    term = weights[a] * line[:, h * LANES : (h + 1) * LANES]
                                    acc[i, h] = acc[i, h] + term if (i, h) in acc else term
                for (i, h), total in acc.items():
                    depth[i, pl.ds(at, 8), h * LANES : (h + 1) * LANES] = total

    def await_halo():
        @pl.when(lat > 0)
        def _():
            rows_down.wait_send()
            comb_down.wait_send()
            rows_up.wait_recv()
            comb_up.wait_recv()
            for r in range(HALO):
                ext[r, :, :cols] = rows_s[r].astype(F32)
                ext[r, :, cols:] = edges_of(comb_s[...].astype(F32), rows - HALO + r)

        @pl.when(lat == 0)
        def _():
            for r in range(HALO):
                ext[r] = jnp.zeros((padded, cols + LANES), F32)

        @pl.when(lat < lat_n - 1)
        def _():
            rows_up.wait_send()
            comb_up.wait_send()
            rows_down.wait_recv()
            comb_down.wait_recv()
            for r in range(HALO):
                ext[rows + HALO + r, :, :cols] = rows_n[r].astype(F32)
                ext[rows + HALO + r, :, cols:] = edges_of(comb_n[...].astype(F32), r)

        @pl.when(lat == lat_n - 1)
        def _():
            for k in range(lon_n - 1, 0, -1):
                fold_copy(k).wait()
            point = lax.broadcasted_iota(jnp.int32, (lon_points, cols + LANES), 0)
            at = lax.broadcasted_iota(jnp.int32, (1, cols + LANES), 1)
            at = jnp.where(at < cols + HALO, at, at - (cols + LANES)) + lon * cols
            mate = fold_ref[:, :1] - at
            mate = jnp.where(mate < 0, mate + lon_points, mate)
            mate = jnp.where(mate < 0, mate + lon_points, mate)
            mate = jnp.where(mate >= lon_points, mate - lon_points, mate)
            pick = jnp.where(point == mate, 1.0, 0.0).astype(BF16)
            for r in range(HALO):
                ext[rows + HALO + r] = jnp.dot(top_all[HALO - 1 - r], pick, preferred_element_type=F32)

    here = pl.ds(pl.multiple_of(lon * cols, LANES), cols)

    def row_at(chunk, q):
        return lax.rem(chunk * lon_n + q + HALO, rows)

    def send_row(chunk, k):
        s = chunk * (lon_n - 1) + lon_n - 1 - k
        return pltpu.make_async_remote_copy(
            res.at[row_at(chunk, target(k))], by_rows.at[chunk, :, here],
            out_send.at[s], out_recv.at[s], device_id={"lon": target(k)})

    def send_back(chunk, k):
        q = target(k)
        s = chunk * (lon_n - 1) + lon_n - 1 - k
        return pltpu.make_async_remote_copy(
            back.at[chunk, :, pl.ds(pl.multiple_of(q * cols, LANES), cols)], spatial.at[chunk * lon_n + lon],
            in_send.at[s], in_recv.at[s], device_id={"lon": q})

    inside = lax.broadcasted_iota(jnp.int32, (padded, 2 * cols), 0) < channels

    def mix_rows(chunk):
        @pl.loop(0, lon_n // 2)
        def _(pair):
            k = lon_n - 1 - 2 * pair
            one, two = row_at(chunk, target(k)), row_at(chunk, target(k - 1))
            x = jnp.concatenate([depth[one], depth[two]], axis=1)
            mean = jnp.sum(x, axis=0, keepdims=True) * (1.0 / channels)
            centred = jnp.where(inside, x - mean, 0.0)
            var = jnp.sum(centred * centred, axis=0, keepdims=True) * (1.0 / channels)
            normed = (centred * lax.rsqrt(var + 1e-06) * gain_col[:, :1]).astype(BF16)
            pre = jnp.dot(w_in_t[...], normed, preferred_element_type=F32)
            hidden = jax.nn.gelu(pre, approximate=True).astype(BF16)
            branch = jnp.dot(w_out_t[...], hidden, preferred_element_type=F32)
            for n, row in enumerate((one, two)):
                wet_row = mask_ref[pl.ds(row, 1), :].astype(F32)
                part = branch[:, n * cols : (n + 1) * cols]
                res[row] = (wet_row * (own[row].astype(F32) + part)).astype(BF16)
            send_row(chunk, k).start()

            @pl.when(pair < lon_n // 2 - 1)
            def _():
                send_row(chunk, k - 1).start()

            @pl.when(pair == lon_n // 2 - 1)
            def _():
                by_rows[chunk, :, here] = res[two]

    def spectral(chunk):
        for k in range(lon_n - 1, 0, -1):
            send_row(chunk, k).wait_recv()
        spectrum = jnp.dot(by_rows[chunk], table_ref[...], preferred_element_type=F32)
        s_re = spectrum[:channels, :modes]
        s_im = spectrum[:channels, modes:]
        g_re = spec_ref[0]
        g_im = spec_ref[1]
        scaled = jnp.concatenate(
            [(g_re * s_re - g_im * s_im).astype(BF16), (g_re * s_im + g_im * s_re).astype(BF16)], axis=1)
        back[chunk, :channels] = lax.dot_general(
            scaled, table_ref[...], (((1,), (1,)), ((), ())), preferred_element_type=F32).astype(BF16)
        for k in range(lon_n - 1, 0, -1):
            send_back(chunk, k).start()
        spatial[chunk * lon_n + lon] = back[chunk, :, here]

    def finish(chunk):
        @pl.loop(0, lon_n)
        def _(k):
            @pl.when(k > 0)
            def _():
                send_back(chunk, k).wait_recv()

            pos = source(k)
            row = row_at(chunk, pos)
            mixed = jnp.dot(mix_t[...], spatial[chunk * lon_n + pos], preferred_element_type=F32)
            wet_row = mask_ref[pl.ds(row, 1), :].astype(F32)
            val = wet_row * (res[row].astype(F32) + mixed)
            flat[0, pl.ds(row, padded, stride=rows), :] = val[:, :LANES]
            flat[1, pl.ds(row, padded, stride=rows), :] = val[:, LANES:]

    halo_done = False
    for chunk in range(per):
        out_rows = [(chunk * lon_n + q + HALO) % rows for q in range(lon_n)]
        if not halo_done and (min(out_rows) < HALO or max(out_rows) >= rows - HALO):
            await_halo()
            halo_done = True
        conv(out_rows)
        mix_rows(chunk)
        if chunk == 1:
            table_copy.wait()
            spec_copy.wait()
        if chunk >= 1:
            spectral(chunk - 1)
    if per == 1:
        table_copy.wait()
        spec_copy.wait()
    for chunk in range(per - 2):
        finish(chunk)
    spectral(per - 1)
    for chunk in range(max(per - 2, 0), per):
        finish(chunk)

    @pl.loop(0, channels)
    def _(c):
        at = pl.multiple_of(c * rows, rows)
        out_ref[c, :, :LANES] = flat[0, pl.ds(at, rows), :].astype(BF16)
        out_ref[c, :, LANES:] = flat[1, pl.ds(at, rows), :].astype(BF16)

    for chunk in range(per):
        for k in range(lon_n - 1, 0, -1):
            send_row(chunk, k).wait_send()
            send_back(chunk, k).wait_send()


def local(lat_n, lon_n, field, land_mask, fold_partner, dw_kernel, norm_gain, w_in, w_out, spec_gain, mix_weight):
    channels, rows, cols = field.shape
    modes = spec_gain.shape[2]
    hid = w_in.shape[1]
    lon_points = cols * lon_n
    padded = -(-channels // 16) * 16
    hid_up = -(-hid // 16) * 16
    table = jnp.asarray(dft_table(lon_points, modes))
    taps = dw_kernel.transpose(1, 2, 0)
    per = rows // lon_n
    sizes = (channels, padded, rows, cols, lat_n, lon_n, modes)
    vmem = pl.BlockSpec(memory_space=pltpu.VMEM)
    hbm = pl.BlockSpec(memory_space=pl.ANY)
    dma = pltpu.SemaphoreType.DMA
    peers = lon_n - 1
    return pl.pallas_call(
        functools.partial(kernel, sizes),
        out_shape=jax.ShapeDtypeStruct(field.shape, BF16),
        in_specs=[vmem] * 8 + [hbm] * 2,
        out_specs=vmem,
        scratch_shapes=[
            pltpu.VMEM((2, padded * rows, LANES), F32),
            pltpu.VMEM((rows + 2 * HALO, padded, cols + LANES), F32),
            pltpu.VMEM((rows, padded, cols), BF16),
            pltpu.VMEM((rows, padded, cols), F32),
            pltpu.VMEM((rows, padded, cols), BF16),
            pltpu.VMEM((per, padded, lon_points), BF16),
            pltpu.VMEM((per, padded, lon_points), BF16),
            pltpu.VMEM((rows, padded, cols), BF16),
            *[pltpu.VMEM((padded, LANES), BF16)] * 6,
            *[pltpu.VMEM((HALO, padded, cols), BF16)] * 2,
            pltpu.VMEM((HALO, padded, lon_points), BF16),
            pltpu.VMEM(spec_gain.shape, F32),
            pltpu.VMEM(table.shape, BF16),
            pltpu.VMEM((TAPS * TAPS, padded, LANES), F32),
            pltpu.VMEM((hid_up, padded), BF16),
            pltpu.VMEM((padded, hid_up), BF16),
            pltpu.VMEM((padded, padded), BF16),
            pltpu.VMEM((padded, LANES), F32),
            *[dma((2,))] * 7,
            *[dma((peers,))] * 2,
            *[dma((peers * per,))] * 4,
        ],
        compiler_params=pltpu.CompilerParams(
            collective_id=0, has_side_effects=True, vmem_limit_bytes=62 * 1024 * 1024),
        name="block",
    )(field, land_mask, fold_partner[None, :], taps, norm_gain[None, :], w_in, w_out.T, mix_weight, spec_gain, table)


def solution(mesh):
    placed = (P(None, "lat", "lon"), P("lat", "lon"), P(), P(), P(), P(), P(), P(), P())
    return jax.shard_map(
        functools.partial(local, mesh.shape["lat"], mesh.shape["lon"]),
        mesh=mesh, in_specs=placed, out_specs=P(None, "lat", "lon"), check_vma=False,
    )
```
